256 devices in a mesh: layer: 64 (over x, z_lo, y, core), tensor: 4 (over z_hi).
Axes of the slice: x: 4, y: 4, z: 8 (z_hi: 4, z_lo: 2; z = z_hi * 2 + z_lo), core: 2. Of those that a mesh axis runs over, the one named last changes fastest.
Arguments:
- gradient: bfloat16 [64, 1024, 8192], P(None, 'tensor', 'layer'), may hold values from -8 to 8
- row_basis: bfloat16 [64, 1024, 256], P('layer', 'tensor'), may hold values from -0.1875 to 0.1875
- column_basis: bfloat16 [64, 8192, 256], P('layer', 'tensor'), may hold values from -0.0625 to 0.0625
- row_eigen: float32 [64, 256], P('layer'), may hold values from 0.01 to 10
- column_eigen: float32 [64, 256], P('layer'), may hold values from 0.01 to 10
- row_escape: float32 [64], P('layer'), may hold values from 0.02 to 0.2
- column_escape: float32 [64], P('layer'), may hold values from 0.02 to 0.2
Outputs:
- update: bfloat16 [64, 1024, 8192], P(None, 'tensor', 'layer')
The draws below stay inside these ranges and needn't reach their ends.
All inputs are finite; a program needn't handle non-finite values.
Results may differ from the reference program's by a relative error of at most 0.0055.
Values may be sent and summed in bfloat16 or wider, within the bound.
A program may use at most 128 MiB of HBM per device.

```python
import math
import jax
import jax.numpy as jnp
from jax import lax

D = 8192
BLK = 1024
K = 256
LAYERS = 64


def draw_gradient(key, part):
    first, second, third, fourth = jax.random.split(jax.random.fold_in(key, 17), 4)
    noise = jax.random.normal(first, (LAYERS, BLK, D), jnp.float32)
    segment = jnp.exp(jax.random.uniform(third, (LAYERS, 1, D // 64), jnp.float32, math.log(0.4), math.log(2.5)))
    segment = jnp.repeat(segment, 64, axis=2)
    rowscale = jnp.exp(jax.random.uniform(second, (LAYERS, BLK, 1), jnp.float32, math.log(0.5), math.log(2.0)))
    values = rowscale * segment * noise
    return jnp.clip(values, -8.0, 8.0).astype(jnp.bfloat16)


def steps_of(stream_key, extent, shards, smallest, largest):
    factor_of = 1.0
    for dim, blocks in shards:
        heights = jax.random.uniform(jax.random.fold_in(jax.random.fold_in(stream_key, 6), dim), (blocks,), jnp.float32, smallest / len(shards), largest / len(shards))
        factor_of = factor_of * jnp.repeat(jnp.exp(heights), extent[dim] // blocks).reshape((-1,) + (1,) * (len(extent) - 1 - dim))
    return factor_of


def scatter_about(rng, dims, scale, bound, shards=(), dtype=jnp.bfloat16):
    values = jax.random.normal(rng, dims, jnp.float32) * scale
    if len(shards) > 0:
        values = steps_of(rng, dims, shards, -0.22, 0.18) * values
    return jnp.clip(values, min=-bound, max=bound).astype(dtype)


def setup_inputs(seed: int = 0) -> dict:
    keys = jax.random.split(jax.random.key(seed), 8)
    return {
        "gradient": draw_gradient(jax.random.fold_in(keys[7], 71), 0),
        "row_basis": scatter_about(keys[1], (LAYERS, BLK, K), BLK ** -0.5, 0.1875, ((0, 64), (1, 4))),
        "column_basis": scatter_about(keys[2], (LAYERS, D, K), D ** -0.5, 0.0625, ((0, 64), (1, 4))),
        "row_eigen": jnp.clip(jnp.exp(math.log(10.0) - 6.9077553 * jax.random.uniform(keys[3], (LAYERS, K), jnp.float32) ** steps_of(keys[3], (LAYERS, K), ((0, 64),), -0.2, 0.2)), 0.01, 10.0),
        "column_eigen": jnp.clip(jnp.exp(math.log(10.0) - 6.9077553 * jax.random.uniform(keys[4], (LAYERS, K), jnp.float32) ** steps_of(keys[4], (LAYERS, K), ((0, 64),), -0.2, 0.2)), 0.01, 10.0),
        "row_escape": jnp.clip(jnp.exp(math.log(0.2) - 2.3025851 * jax.random.uniform(keys[5], (LAYERS,), jnp.float32) ** steps_of(keys[5], (LAYERS,), ((0, 64),), -0.2, 0.2)), 0.02, 0.2),
        "column_escape": jnp.clip(jnp.exp(math.log(0.2) - 2.3025851 * jax.random.uniform(keys[6], (LAYERS,), jnp.float32) ** steps_of(keys[6], (LAYERS,), ((0, 64),), -0.2, 0.2)), 0.02, 0.2),
    }


def one_layer(operands):
    block_grad, basis_rows, basis_columns, eigen_rows, eigen_columns, escape_rows, escape_columns = operands
    row_base = escape_rows ** (-0.25)
    column_base = escape_columns ** (-0.25)
    row_coef = (eigen_rows + escape_rows) ** (-0.25) - row_base
    column_coef = (eigen_columns + escape_columns) ** (-0.25) - column_base
    projected = jnp.dot(basis_rows.T, block_grad, preferred_element_type=jnp.float32)
    scaled = (row_coef[:, None] * projected).astype(jnp.bfloat16)
    core = jnp.dot(scaled, basis_columns, preferred_element_type=jnp.float32).astype(jnp.bfloat16)
    middle = jnp.dot(block_grad, basis_columns, preferred_element_type=jnp.float32)
    left_factor = ((row_base * middle + jnp.dot(basis_rows, core, preferred_element_type=jnp.float32)) * column_coef[None, :]).astype(jnp.bfloat16)
    raw_update = row_base * column_base * block_grad.astype(jnp.float32)
    raw_update = raw_update + column_base * jnp.dot(basis_rows, scaled, preferred_element_type=jnp.float32)
    raw_update = raw_update + jnp.dot(left_factor, basis_columns.T, preferred_element_type=jnp.float32)
    grad_sq = jnp.sum(jnp.square(block_grad.astype(jnp.float32)))
    update_sq = jnp.sum(jnp.square(raw_update))
    return (raw_update * jnp.sqrt((grad_sq + 1.0) / (update_sq + 1.0))).astype(jnp.bfloat16)

def reference(gradient, row_basis, column_basis, row_eigen, column_eigen, row_escape, column_escape):
    return lax.map(one_layer, (gradient, row_basis, column_basis, row_eigen, column_eigen, row_escape, column_escape))
```

```python
import jax
import jax.numpy as jnp
from jax import lax
from jax.experimental import pallas as pl
from jax.experimental.pallas import tpu as pltpu
from jax.sharding import PartitionSpec as P

MESH = pl.DeviceIdType.MESH
F32 = jnp.float32
BF16 = jnp.bfloat16


def layer_at(x, y, zlo, core):
    return ((x * 2 + zlo) * 4 + y) * 2 + core


def remote(src, dst, send, recv, layer, tensor):
    return pltpu.make_async_remote_copy(
        src_ref=src,
        dst_ref=dst,
        send_sem=send,
        recv_sem=recv,
        device_id=(layer, tensor),
        device_id_type=MESH,
    )


def wait_bytes(ref, sem):
    pltpu.make_async_copy(ref, ref, sem).wait()


def inverse_fourth_root(value):
    return lax.rsqrt(jnp.sqrt(value))


def fold(value):
    rows, cols = value.shape
    parts = jnp.sum((value * value).reshape(rows // 8, 8, cols), axis=0)
    return sum(parts[:, c : c + 128] for c in range(0, cols, 128))


def kernel(
    row_esc,
    col_esc,
    grad,
    row_own,
    cols,
    row_eig,
    col_eig,
    out,
    block,
    mid,
    rows,
    rows_t,
    coef_t,
    scaled,
    middle,
    mid_send,
    mid_recv,
    mid_all,
    left,
    raw,
    ready,
    norm_send,
    norm_recv,
    grad_acc,
    sent,
    relay_sem,
    block_sem,
    rows_sem,
    rows_sent,
    part_sem,
    part_sent,
    full_sem,
    full_sent,
    norm_sem,
    norm_sent,
    out_sem,
    out_sent,
):
    me, t = lax.axis_index("layer"), lax.axis_index("tensor")
    x, zlo, y, core = me // 16, lax.rem(me // 8, 2), lax.rem(me // 2, 4), lax.rem(me, 2)
    z = 2 * t + zlo
    my_block = lax.rem(me, 16)
    home = t == x

    barrier = pltpu.get_barrier_semaphore()

    def greet_plane(i, carry):
        d = lax.rem((x * 4 + y) * 2 + core + i, 32)
        pl.semaphore_signal(
            barrier,
            inc=1,
            device_id=(layer_at(d // 8, lax.rem(d // 2, 4), zlo, lax.rem(d, 2)), t),
            device_id_type=MESH,
        )
        return carry

    def greet_ring(i, carry):
        dz = lax.rem(z + i, 8)
        pl.semaphore_signal(
            barrier,
            inc=1,
            device_id=(layer_at(x, y, lax.rem(dz, 2), core), dz // 2),
            device_id_type=MESH,
        )
        return carry

    lax.fori_loop(1, 32, greet_plane, 0)
    lax.fori_loop(1, 8, greet_ring, 0)
    pl.semaphore_wait(barrier, 38)

    def offsets(k):
        a = lax.rem(k + 1, 4)
        return a, lax.rem(k // 4 + a, 4)

    def block_rows(ref, index, part):
        return ref.at[index, pl.ds(pl.multiple_of(part * 256, 256), 256)]

    def scatter_plane(k, carry):
        kk, dest_core = lax.rem(k, 16), k // 16
        a, b = offsets(kk)
        dx, dy = lax.rem(x + a, 4), lax.rem(y + b, 4)
        mine = (dx == x) & (dy == y) & (dest_core == core)
        relay = layer_at(dx, dy, zlo, dest_core)
        slot = core * 16 + kk
        for dz in range(2):
            layer = layer_at(dx, dy, dz, dest_core)
            final = 2 * x + dz == z
            target = block_rows(block, my_block, t)

            @pl.when(jnp.logical_not(mine) & jnp.logical_not(final))
            def _():
                remote(
                    grad.at[layer], mid.at[slot, dz], sent, relay_sem.at[slot, dz], relay, t
                ).start()

            @pl.when(jnp.logical_not(mine) & final)
            def _():
                remote(grad.at[layer], target, sent, block_sem.at[my_block], relay, t).start()

            @pl.when(mine & jnp.logical_not(final))
            def _():
                remote(grad.at[layer], target, sent, block_sem.at[my_block], layer, x).start()

            @pl.when(mine & final)
            def _():
                pltpu.make_async_copy(grad.at[layer], target, block_sem.at[my_block]).start()

        return carry

    lax.fori_loop(0, 32, scatter_plane, 0)

    pltpu.make_async_copy(row_own, rows.at[t], rows_sem).start()
    for o in range(1, 4):
        remote(row_own, rows.at[t], rows_sent, rows_sem, me, lax.rem(t + o, 4)).start()

    def forward(k, carry):
        kk, source_core = k // 2, lax.rem(core + k, 2)
        a, b = offsets(kk)
        sx, sy = lax.rem(x - a + 4, 4), lax.rem(y - b + 4, 4)
        mine = (sx == x) & (sy == y) & (source_core == core)
        slot = source_core * 16 + kk
        index = zlo * 8 + sy * 2 + source_core
        for dz in range(2):

            @pl.when(jnp.logical_not(mine) & (2 * sx + dz != z))
            def _():
                held = mid.at[slot, dz]
                wait_bytes(held, relay_sem.at[slot, dz])
                remote(
                    held,
                    block_rows(block, index, t),
                    sent,
                    block_sem.at[index],
                    layer_at(x, y, dz, core),
                    sx,
                ).start()

        return carry

    lax.fori_loop(0, 32, forward, 0)

    row_e = jnp.full((1, 256), row_esc[0], F32)
    col_e = jnp.full((1, 256), col_esc[0], F32)
    row_base, col_base = inverse_fourth_root(row_e), inverse_fourth_root(col_e)
    row_coef = inverse_fourth_root(row_eig[...] + row_e) - row_base
    col_coef = inverse_fourth_root(col_eig[...] + col_e) - col_base
    coef_t[...] = jnp.transpose(jnp.broadcast_to(row_coef, (256, 256)))

    wait_bytes(rows, rows_sem)
    for r in range(4):
        rows_t[:, 256 * r : 256 * (r + 1)] = jnp.transpose(rows[r].astype(F32)).astype(BF16)

    middle[...] = jnp.zeros_like(middle)
    grad_acc[...] = jnp.zeros_like(grad_acc)
    shift = lax.rem(x - t + 4, 4)

    def project(i, carry):
        sy = lax.rem(y - shift - i // 2 + 8, 4)
        p = lax.rem(i, 2) * 4 + sy
        for half in range(2):
            wait_bytes(block.at[2 * p + half], block_sem.at[2 * p + half])
        pair = jnp.concatenate([block[2 * p], block[2 * p + 1]], axis=1)
        proj = jnp.dot(rows_t[...], pair, preferred_element_type=F32)
        scaled[p] = (coef_t[...] * proj).astype(BF16)
        column = cols[pl.ds(pl.multiple_of(p * 256, 256), 256), :]
        for r in range(4):
            piece = pair[256 * r : 256 * (r + 1)]
            middle[r] += jnp.dot(piece, column, preferred_element_type=F32)
            grad_acc[...] += fold(piece.astype(F32))
        return carry

    lax.fori_loop(0, 8, project, 0)

    for r in range(4):
        mid_send[r] = middle[r].astype(BF16)
    for o in range(1, 4):
        peer = lax.rem(t + o, 4)
        remote(mid_send.at[peer], mid_recv.at[3 - o], part_sent, part_sem, me, peer).start()
    wait_bytes(mid_recv, part_sem)
    total = middle[t]
    for o in range(3):
        total = total + mid_recv[o].astype(F32)
    mid_all[t] = total.astype(BF16)
    for o in range(1, 4):
        peer = lax.rem(t + o, 4)
        remote(mid_all.at[t], mid_all.at[t], full_sent, full_sem, me, peer).start()
    wait_bytes(mid_recv, full_sem)

    core_mat = jnp.zeros((256, 256), F32)
    for r in range(4):
        core_mat += jnp.dot(
            rows_t[:, 256 * r : 256 * (r + 1)], mid_all[r], preferred_element_type=F32
        )
    core_mat = (coef_t[...] * core_mat).astype(BF16)
    for r in range(4):
        mixed = row_base * mid_all[r].astype(F32) + jnp.dot(
            rows[r], core_mat, preferred_element_type=F32
        )
        left[r] = (mixed * col_coef).astype(BF16)

    both_base = row_base * col_base
    norm_send[0] = grad_acc[...]
    norm_send[1] = jnp.zeros((8, 128), F32)

    def update(p, carry):
        column = cols[pl.ds(pl.multiple_of(p * 256, 256), 256), :]
        for r in range(4):
            span = slice(256 * r, 256 * (r + 1))
            value = jnp.dot(rows[r], scaled[p], preferred_element_type=F32) * col_base
            value += lax.dot_general(
                left[r], column, (((1,), (1,)), ((), ())), preferred_element_type=F32
            )
            held = jnp.concatenate([block[2 * p, span], block[2 * p + 1, span]], axis=1)
            value += both_base * held.astype(F32)
            raw[p, span] = value
            norm_send[1] += fold(value)
        return carry

    lax.fori_loop(0, 8, update, 0)

    for o in range(1, 4):
        remote(
            norm_send, norm_recv.at[3 - o], norm_sent, norm_sem, me, lax.rem(t + o, 4)
        ).start()
    wait_bytes(norm_recv, norm_sem)
    sums = norm_send[...] + norm_recv[0] + norm_recv[1] + norm_recv[2]
    grad_sq = jnp.sum(sums[0], keepdims=True)
    update_sq = jnp.sum(sums[1], keepdims=True)
    factor = jnp.sqrt((grad_sq + 1.0) / (update_sq + 1.0))

    def give(i, carry):
        def order(k):
            return lax.rem(zlo + k, 2) * 4 + lax.rem(y + k // 2, 4)

        @pl.when(i < 8)
        def _():
            p = order(i)
            for half in range(2):
                ready[2 * p + half] = (
                    raw[p, :, 128 * half : 128 * (half + 1)] * factor
                ).astype(BF16)

        @pl.when(i > 0)
        def _():
            p = order(i - 1)
            for h in range(2):
                index = 2 * p + lax.rem(core + h, 2)
                layer = t * 16 + index
                for o in range(4):
                    part = lax.rem(t + o + 1, 4)
                    piece = block_rows(ready, index, part)
                    own = (layer == me) & (part == t)

                    @pl.when(jnp.logical_not(own))
                    def _():
                        remote(piece, out.at[me], out_sent, out_sem, layer, part).start()

                    @pl.when(own)
                    def _():
                        pltpu.make_async_copy(piece, out.at[me], out_sem).start()

        return carry

    lax.fori_loop(0, 9, give, 0)

    wait_bytes(raw.at[pl.ds(0, 7)], sent)
    wait_bytes(raw.at[7, pl.ds(0, 384)], sent)
    wait_bytes(rows.at[pl.ds(0, 3)], rows_sent)
    wait_bytes(mid_recv, part_sent)
    wait_bytes(mid_recv, full_sent)
    wait_bytes(norm_recv, norm_sent)

    @pl.when(home)
    def _():
        wait_bytes(out.at[pl.ds(0, 63)], out_sent)

    @pl.when(jnp.logical_not(home))
    def _():
        wait_bytes(out, out_sent)

    wait_bytes(out, out_sem)


def body(gradient, row_basis, column_basis, row_eigen, column_eigen, row_escape, column_escape):
    dma = pltpu.SemaphoreType.DMA
    vmem = pl.BlockSpec(memory_space=pltpu.VMEM)
    smem = pl.BlockSpec(memory_space=pltpu.SMEM)
    hbm = pl.BlockSpec(memory_space=pltpu.HBM)
    return pl.pallas_call(
        kernel,
        out_shape=jax.ShapeDtypeStruct((64, 256, 128), BF16),
        in_specs=[smem, smem, hbm, hbm, vmem, vmem, vmem],
        out_specs=hbm,
        scratch_shapes=[
            pltpu.VMEM((16, 1024, 128), BF16),
            pltpu.VMEM((32, 2, 256, 128), BF16),
            pltpu.VMEM((4, 256, 256), BF16),
            pltpu.VMEM((256, 1024), BF16),
            pltpu.VMEM((256, 256), F32),
            pltpu.VMEM((8, 256, 256), BF16),
            pltpu.VMEM((4, 256, 256), F32),
            pltpu.VMEM((4, 256, 256), BF16),
            pltpu.VMEM((3, 256, 256), BF16),
            pltpu.VMEM((4, 256, 256), BF16),
            pltpu.VMEM((4, 256, 256), BF16),
            pltpu.VMEM((8, 1024, 256), F32),
            pltpu.VMEM((16, 1024, 128), BF16),
            pltpu.VMEM((2, 8, 128), F32),
            pltpu.VMEM((3, 2, 8, 128), F32),
            pltpu.VMEM((8, 128), F32),
            dma,
            dma((32, 2)),
            dma((16,)),
            dma,
            dma,
            dma,
            dma,
            dma,
            dma,
            dma,
            dma,
            dma,
            dma,
        ],
        compiler_params=pltpu.CompilerParams(
            collective_id=0, has_side_effects=True, vmem_limit_bytes=56 * 1024 * 1024
        ),
        name="sketchy",
    )(
        row_escape,
        column_escape,
        gradient,
        row_basis.reshape(256, 256),
        column_basis.reshape(2048, 256),
        row_eigen,
        column_eigen,
    )


def solution(mesh):
    in_specs = (
        P(None, "tensor", "layer"),
        P("layer", "tensor", None),
        P("layer", "tensor", None),
        P("layer", None),
        P("layer", None),
        P("layer"),
        P("layer"),
    )
    out_specs = P(None, "tensor", "layer")
    return jax.shard_map(body, mesh=mesh, in_specs=in_specs, out_specs=out_specs, check_vma=False)
```

```python
import jax
import jax.numpy as jnp
from jax import lax
from jax.experimental import pallas as pl
from jax.experimental.pallas import tpu as pltpu
from jax.sharding import PartitionSpec as P

MESH = pl.DeviceIdType.MESH
GO_AFTER = 4
EARLY, LATE = 2, 6
F32 = jnp.float32
BF16 = jnp.bfloat16


def layer_at(x, y, zlo, core):
    return ((x * 2 + zlo) * 4 + y) * 2 + core


def remote(src, dst, send, recv, layer, tensor):
    return pltpu.make_async_remote_copy(
        src_ref=src,
        dst_ref=dst,
        send_sem=send,
        recv_sem=recv,
        device_id=(layer, tensor),
        device_id_type=MESH,
    )


def wait_bytes(ref, sem):
    pltpu.make_async_copy(ref, ref, sem).wait()


def inverse_fourth_root(value):
    return lax.rsqrt(jnp.sqrt(value))


def fold(value):
    rows, cols = value.shape
    parts = jnp.sum((value * value).reshape(rows // 8, 8, cols), axis=0)
    return sum(parts[:, c : c + 128] for c in range(0, cols, 128))


def kernel(
    row_esc,
    col_esc,
    grad,
    row_own,
    cols_in,
    row_eig,
    col_eig,
    out,
    block,
    mid,
    rows,
    rows_t,
    coef_t,
    scaled,
    middle,
    mid_far,
    mid_via,
    mid_send,
    mid_recv,
    mid_all,
    left,
    ready,
    factor_out,
    factor_in,
    norm_send,
    norm_recv,
    grad_acc,
    cols,
    sent,
    relay_sem,
    block_sem,
    rows_sem,
    rows_sent,
    part_sem,
    part_sent,
    full_sem,
    full_sent,
    norm_sem,
    norm_sent,
    out_sem,
    out_sent,
    factor_sem,
    factor_sent,
    go_sem,
    cols_sem,
    own_sem,
    rows_last,
    rows_sent2,
    far_sem,
    far_sent,
    full_last,
    full_sent2,
):
    me, t = lax.axis_index("layer"), lax.axis_index("tensor")
    x, zlo, y, core = me // 16, lax.rem(me // 8, 2), lax.rem(me // 2, 4), lax.rem(me, 2)
    z = 2 * t + zlo
    my_block = lax.rem(me, 16)
    home = t == x

    barrier = pltpu.get_barrier_semaphore()

    def greet_plane(i, carry):
        d = lax.rem((x * 4 + y) * 2 + core + i, 32)
        pl.semaphore_signal(
            barrier,
            inc=1,
            device_id=(layer_at(d // 8, lax.rem(d // 2, 4), zlo, lax.rem(d, 2)), t),
            device_id_type=MESH,
        )
        return carry

    def greet_ring(i, carry):
        dz = lax.rem(z + i, 8)
        pl.semaphore_signal(
            barrier,
            inc=1,
            device_id=(layer_at(x, y, lax.rem(dz, 2), core), dz // 2),
            device_id_type=MESH,
        )
        return carry

    lax.fori_loop(1, 32, greet_plane, 0)
    lax.fori_loop(1, 8, greet_ring, 0)
    pl.semaphore_wait(barrier, 38)

    up, down, across = lax.rem(t + 1, 4), lax.rem(t + 3, 4), lax.rem(t + 2, 4)

    def pass_round(source, blocks, first, second, first_sent, second_sent):
        remote(source, blocks.at[t], first_sent, first.at[0], me, up).start()
        remote(source, blocks.at[t], first_sent, first.at[1], me, down).start()

        def pass_on():
            wait_bytes(blocks.at[down], first.at[0])
            half = blocks.at[down, pl.ds(0, 128)]
            remote(half, half, second_sent, second, me, up).start()
            wait_bytes(blocks.at[up], first.at[1])
            half = blocks.at[up, pl.ds(128, 128)]
            remote(half, half, second_sent, second, me, down).start()

        return pass_on

    own_rows = pltpu.make_async_copy(row_own, rows.at[t], own_sem)
    own_rows.start()
    pass_rows_on = pass_round(row_own, rows, rows_sem, rows_last, rows_sent, rows_sent2)

    pltpu.make_async_copy(cols_in, cols, cols_sem).start()

    def offsets(k):
        a = lax.rem(k + 1, 4)
        return a, lax.rem(k // 4 + a, 4)

    def block_rows(ref, index, part):
        return ref.at[index, pl.ds(pl.multiple_of(part * 256, 256), 256)]

    def scatter_plane(k, carry):
        kk, dest_core = lax.rem(k, 16), k // 16
        a, b = offsets(kk)
        dx, dy = lax.rem(x + a, 4), lax.rem(y + b, 4)
        mine = (dx == x) & (dy == y) & (dest_core == core)
        relay = layer_at(dx, dy, zlo, dest_core)
        slot = core * 16 + kk
        for dz in range(2):
            layer = layer_at(dx, dy, dz, dest_core)
            final = 2 * x + dz == z
            target = block_rows(block, my_block, t)

            @pl.when(jnp.logical_not(mine) & jnp.logical_not(final))
            def _():
                remote(
                    grad.at[layer], mid.at[slot, dz], sent, relay_sem.at[slot, dz], relay, t
                ).start()

            @pl.when(jnp.logical_not(mine) & final)
            def _():
                remote(grad.at[layer], target, sent, block_sem.at[my_block], relay, t).start()

            @pl.when(mine & jnp.logical_not(final))
            def _():
                remote(grad.at[layer], target, sent, block_sem.at[my_block], layer, x).start()

            @pl.when(mine & final)
            def _():
                pltpu.make_async_copy(grad.at[layer], target, block_sem.at[my_block]).start()

        return carry

    lax.fori_loop(0, 32, scatter_plane, 0)

    def forward(k, carry):
        kk, source_core = k // 2, lax.rem(core + k, 2)
        a, b = offsets(kk)
        sx, sy = lax.rem(x - a + 4, 4), lax.rem(y - b + 4, 4)
        mine = (sx == x) & (sy == y) & (source_core == core)
        slot = source_core * 16 + kk
        index = zlo * 8 + sy * 2 + source_core
        for dz in range(2):

            @pl.when(jnp.logical_not(mine) & (2 * sx + dz != z))
            def _():
                held = mid.at[slot, dz]
                wait_bytes(held, relay_sem.at[slot, dz])
                remote(
                    held,
                    block_rows(block, index, t),
                    sent,
                    block_sem.at[index],
                    layer_at(x, y, dz, core),
                    sx,
                ).start()

        return carry

    lax.fori_loop(0, (1 - core) * 8, forward, 0)
    pass_rows_on()
    @pl.when(core == 1)
    def _():
        pl.semaphore_wait(go_sem, 1)

    lax.fori_loop((1 - core) * 8, 32, forward, 0)

    row_e = jnp.full((1, 256), row_esc[0], F32)
    col_e = jnp.full((1, 256), col_esc[0], F32)
    row_base, col_base = inverse_fourth_root(row_e), inverse_fourth_root(col_e)
    row_coef = inverse_fourth_root(row_eig[...] + row_e) - row_base
    col_coef = inverse_fourth_root(col_eig[...] + col_e) - col_base
    coef_t[...] = jnp.transpose(jnp.broadcast_to(row_coef, (256, 256)))

    own_rows.wait()
    wait_bytes(rows.at[across], rows_last)
    wait_bytes(cols, cols_sem)
    for r in range(4):
        rows_t[:, 256 * r : 256 * (r + 1)] = jnp.transpose(rows[r].astype(F32)).astype(BF16)

    middle[...] = jnp.zeros_like(middle)
    grad_acc[...] = jnp.zeros_like(grad_acc)
    shift = lax.rem(x - t + 4, 4)

    def project(i, carry):
        sy = lax.rem(y - shift - i // 2 + 8, 4)
        p = lax.rem(i, 2) * 4 + sy
        for half in range(2):
            wait_bytes(block.at[2 * p + half], block_sem.at[2 * p + half])
        pair = jnp.concatenate([block[2 * p], block[2 * p + 1]], axis=1)
        proj = jnp.dot(rows_t[...], pair, preferred_element_type=F32)
        scaled[p] = (coef_t[...] * proj).astype(BF16)
        column = cols[pl.ds(pl.multiple_of(p * 256, 256), 256), :]
        for r in range(4):
            piece = pair[256 * r : 256 * (r + 1)]
            middle[r] += jnp.dot(piece, column, preferred_element_type=F32)
            grad_acc[...] += fold(piece.astype(F32))

        @pl.when((core == 0) & (i == GO_AFTER))
        def _():
            pl.semaphore_signal(go_sem, inc=1, device_id=(me + 1, t), device_id_type=MESH)

        return carry

    lax.fori_loop(0, 8, project, 0)

    far = middle[across].astype(BF16)
    mid_far[...] = far
    remote(mid_far.at[pl.ds(0, 128)], mid_via.at[0], far_sent, far_sem.at[0], me, down).start()
    remote(mid_far.at[pl.ds(128, 128)], mid_via.at[1], far_sent, far_sem.at[1], me, up).start()
    wait_bytes(mid_via.at[0], far_sem.at[0])
    wait_bytes(mid_via.at[1], far_sem.at[1])
    mid_send[0, 0:128] = (middle[down, 0:128] + mid_via[0].astype(F32)).astype(BF16)
    mid_send[0, 128:256] = middle[down, 128:256].astype(BF16)
    mid_send[1, 0:128] = middle[up, 0:128].astype(BF16)
    mid_send[1, 128:256] = (middle[up, 128:256] + mid_via[1].astype(F32)).astype(BF16)
    remote(mid_send.at[0], mid_recv.at[0], part_sent, part_sem, me, down).start()
    remote(mid_send.at[1], mid_recv.at[1], part_sent, part_sem, me, up).start()
    wait_bytes(mid_recv, part_sem)
    mid_all[t] = (middle[t] + mid_recv[0].astype(F32) + mid_recv[1].astype(F32)).astype(BF16)
    pass_middle_on = pass_round(mid_all.at[t], mid_all, full_sem, full_last, full_sent, full_sent2)
    pass_middle_on()
    wait_bytes(mid_all.at[across], full_last)

    core_mat = jnp.zeros((256, 256), F32)
    for r in range(4):
        core_mat += jnp.dot(
            rows_t[:, 256 * r : 256 * (r + 1)], mid_all[r], preferred_element_type=F32
        )
    core_mat = (coef_t[...] * core_mat).astype(BF16)
    for r in range(4):
        mixed = row_base * mid_all[r].astype(F32) + jnp.dot(
            rows[r], core_mat, preferred_element_type=F32
        )
        left[r] = (mixed * col_coef).astype(BF16)

    both_base = row_base * col_base
    norm_send[0] = grad_acc[...]
    norm_send[1] = jnp.zeros((8, 128), F32)

    def order(k):
        return lax.rem(zlo + k, 2) * 4 + lax.rem(y + k // 2, 4)

    def send_pair(i, carry):
        p = order(i)
        for h in range(2):
            index = 2 * p + lax.rem(core + h, 2)
            layer = t * 16 + index
            for o in range(4):
                part = lax.rem(t + o + 1, 4)
                piece = block_rows(ready, index, part)
                own = (layer == me) & (part == t)

                @pl.when(jnp.logical_not(own))
                def _():
                    remote(piece, out.at[me], out_sent, out_sem.at[me], layer, part).start()

                @pl.when(own)
                def _():
                    pltpu.make_async_copy(piece, out.at[me], out_sem.at[me]).start()

        return carry

    def update(i, carry):
        p = order(i)
        column = cols[pl.ds(pl.multiple_of(p * 256, 256), 256), :]
        for r in range(4):
            span = slice(256 * r, 256 * (r + 1))
            value = jnp.dot(rows[r], scaled[p], preferred_element_type=F32) * col_base
            value += lax.dot_general(
                left[r], column, (((1,), (1,)), ((), ())), preferred_element_type=F32
            )
            held = jnp.concatenate([block[2 * p, span], block[2 * p + 1, span]], axis=1)
            value += both_base * held.astype(F32)
            ready[2 * p, span] = value[:, :128].astype(BF16)
            ready[2 * p + 1, span] = value[:, 128:].astype(BF16)
            norm_send[1] += fold(value)

        @pl.when((i > 0) & (i <= EARLY))
        def _():
            send_pair(i - 1, 0)

        return carry

    lax.fori_loop(0, 8, update, 0)
    for o in range(1, 4):
        remote(
            norm_send, norm_recv.at[3 - o], norm_sent, norm_sem, me, lax.rem(t + o, 4)
        ).start()
    lax.fori_loop(EARLY, LATE, send_pair, 0)
    wait_bytes(norm_recv, norm_sem)
    sums = norm_send[...] + norm_recv[0] + norm_recv[1] + norm_recv[2]
    grad_sq = jnp.sum(sums[0], keepdims=True)
    update_sq = jnp.sum(sums[1], keepdims=True)
    factor = jnp.sqrt((grad_sq + 1.0) / (update_sq + 1.0))
    factor_out[...] = jnp.broadcast_to(factor, (8, 128))
    wait_bytes(norm_recv, norm_sent)

    def give(i, carry):
        layer, part = t * 16 + lax.rem(my_block + i // 4, 16), lax.rem(t + i + 1, 4)
        own = (layer == me) & (part == t)

        @pl.when(jnp.logical_not(own))
        def _():
            remote(
                factor_out.at[pl.ds(0, 1)],
                factor_in.at[me, pl.ds(0, 1)],
                factor_sent,
                factor_sem.at[me],
                layer,
                part,
            ).start()

        @pl.when(own)
        def _():
            pltpu.make_async_copy(
                factor_out.at[pl.ds(0, 1)], factor_in.at[me, pl.ds(0, 1)], factor_sem.at[me]
            ).start()

        return carry

    lax.fori_loop(0, 64, give, 0)
    lax.fori_loop(LATE, 8, send_pair, 0)

    def scale(i, carry):
        layer = lax.rem(i, 32) * 2 + i // 32
        wait_bytes(out.at[layer], out_sem.at[layer])
        wait_bytes(factor_in.at[layer, pl.ds(0, 1)], factor_sem.at[layer])
        out[layer] = (out[layer].astype(F32) * factor_in[layer, 0:1]).astype(BF16)
        return carry

    lax.fori_loop(0, 64, scale, 0)
    wait_bytes(mid, sent)
    wait_bytes(mid.at[pl.ds(0, 27)], sent)
    wait_bytes(rows.at[pl.ds(0, 2)], rows_sent)
    wait_bytes(rows.at[0], rows_sent2)
    wait_bytes(mid_far, far_sent)
    wait_bytes(mid_recv, part_sent)
    wait_bytes(mid_recv, full_sent)
    wait_bytes(mid_far, full_sent2)

    @pl.when(home)
    def _():
        wait_bytes(out.at[pl.ds(0, 63)], out_sent)
        wait_bytes(factor_in.at[pl.ds(0, 63), pl.ds(0, 1)], factor_sent)

    @pl.when(jnp.logical_not(home))
    def _():
        wait_bytes(out, out_sent)
        wait_bytes(factor_in.at[:, pl.ds(0, 1)], factor_sent)


def body(gradient, row_basis, column_basis, row_eigen, column_eigen, row_escape, column_escape):
    dma = pltpu.SemaphoreType.DMA
    vmem = pl.BlockSpec(memory_space=pltpu.VMEM)
    smem = pl.BlockSpec(memory_space=pltpu.SMEM)
    hbm = pl.BlockSpec(memory_space=pltpu.HBM)
    return pl.pallas_call(
        kernel,
        out_shape=pltpu.VMEM((64, 256, 128), BF16),
        in_specs=[smem, smem, hbm, hbm, hbm, vmem, vmem],
        out_specs=vmem,
        scratch_shapes=[
            pltpu.VMEM((16, 1024, 128), BF16),
            pltpu.VMEM((32, 2, 256, 128), BF16),
            pltpu.VMEM((4, 256, 256), BF16),
            pltpu.VMEM((256, 1024), BF16),
            pltpu.VMEM((256, 256), F32),
            pltpu.VMEM((8, 256, 256), BF16),
            pltpu.VMEM((4, 256, 256), F32),
            pltpu.VMEM((256, 256), BF16),
            pltpu.VMEM((2, 128, 256), BF16),
            pltpu.VMEM((2, 256, 256), BF16),
            pltpu.VMEM((2, 256, 256), BF16),
            pltpu.VMEM((4, 256, 256), BF16),
            pltpu.VMEM((4, 256, 256), BF16),
            pltpu.VMEM((16, 1024, 128), BF16),
            pltpu.VMEM((8, 128), F32),
            pltpu.VMEM((64, 8, 128), F32),
            pltpu.VMEM((2, 8, 128), F32),
            pltpu.VMEM((3, 2, 8, 128), F32),
            pltpu.VMEM((8, 128), F32),
            pltpu.VMEM((2048, 256), BF16),
            dma,
            dma((32, 2)),
            dma((16,)),
            dma((2,)),
            dma,
            dma,
            dma,
            dma((2,)),
            dma,
            dma,
            dma,
            dma((64,)),
            dma,
            dma((64,)),
            dma,
            pltpu.SemaphoreType.REGULAR,
            dma,
            dma,
            dma,
            dma,
            dma((2,)),
            dma,
            dma,
            dma,
        ],
        compiler_params=pltpu.CompilerParams(
            collective_id=0, has_side_effects=True, vmem_limit_bytes=56 * 1024 * 1024
        ),
        name="sketchy",
    )(
        row_escape,
        column_escape,
        gradient,
        row_basis.reshape(256, 256),
        column_basis.reshape(2048, 256),
        row_eigen,
        column_eigen,
    )


def solution(mesh):
    in_specs = (
        P(None, "tensor", "layer"),
        P("layer", "tensor", None),
        P("layer", "tensor", None),
        P("layer", None),
        P("layer", None),
        P("layer"),
        P("layer"),
    )
    out_specs = P(None, "tensor", "layer")
    return jax.shard_map(body, mesh=mesh, in_specs=in_specs, out_specs=out_specs, check_vma=False)
```

```python
import jax
import jax.numpy as jnp
from jax import lax
from jax.experimental import pallas as pl
from jax.experimental.pallas import tpu as pltpu
from jax.sharding import PartitionSpec as P

MESH = pl.DeviceIdType.MESH
GO_AFTER = 4
EARLY, LATE = 3, 7
F32 = jnp.float32
BF16 = jnp.bfloat16


def layer_at(x, y, zlo, core):
    return ((x * 2 + zlo) * 4 + y) * 2 + core


def remote(src, dst, send, recv, layer, tensor):
    return pltpu.make_async_remote_copy(
        src_ref=src,
        dst_ref=dst,
        send_sem=send,
        recv_sem=recv,
        device_id=(layer, tensor),
        device_id_type=MESH,
    )


def wait_bytes(ref, sem):
    pltpu.make_async_copy(ref, ref, sem).wait()


def inverse_fourth_root(value):
    return lax.rsqrt(jnp.sqrt(value))


def fold(value):
    rows, cols = value.shape
    parts = jnp.sum((value * value).reshape(rows // 8, 8, cols), axis=0)
    return sum(parts[:, c : c + 128] for c in range(0, cols, 128))


def kernel(
    row_esc_in,
    col_esc_in,
    grad,
    row_own,
    cols_in,
    row_eig_in,
    col_eig_in,
    out,
    block,
    mid,
    rows,
    rows_t,
    coef_t,
    scaled,
    middle,
    mid_far,
    mid_via,
    mid_send,
    mid_recv,
    mid_all,
    left,
    ready,
    factor_out,
    factor_in,
    norm_send,
    norm_recv,
    grad_acc,
    cols,
    row_esc,
    col_esc,
    row_eig,
    col_eig,
    sent,
    relay_sem,
    block_sem,
    rows_sem,
    rows_sent,
    part_sem,
    part_sent,
    full_sem,
    full_sent,
    norm_sem,
    norm_sent,
    out_sem,
    out_sent,
    factor_sem,
    factor_sent,
    go_sem,
    cols_sem,
    own_sem,
    rows_last,
    rows_sent2,
    far_sem,
    far_sent,
    full_last,
    full_sent2,
    small_sem,
):
    me, t = lax.axis_index("layer"), lax.axis_index("tensor")
    x, zlo, y, core = me // 16, lax.rem(me // 8, 2), lax.rem(me // 2, 4), lax.rem(me, 2)
    z = 2 * t + zlo
    my_block = lax.rem(me, 16)
    home = t == x
    my_group = ((1 - core) * 4 + x) * 2 + zlo

    barrier = pltpu.get_barrier_semaphore()

    def greet_plane(i, carry):
        d = lax.rem((x * 4 + y) * 2 + core + i, 32)
        pl.semaphore_signal(
            barrier,
            inc=1,
            device_id=(layer_at(d // 8, lax.rem(d // 2, 4), zlo, lax.rem(d, 2)), t),
            device_id_type=MESH,
        )
        return carry

    def greet_ring(i, carry):
        dz = lax.rem(z + i, 8)
        pl.semaphore_signal(
            barrier,
            inc=1,
            device_id=(layer_at(x, y, lax.rem(dz, 2), core), dz // 2),
            device_id_type=MESH,
        )
        return carry

    lax.fori_loop(1, 8, greet_ring, 0, unroll=True)
    lax.fori_loop(1, 32, greet_plane, 0, unroll=True)
    pl.semaphore_wait(barrier, 38)

    up, down, across = lax.rem(t + 1, 4), lax.rem(t + 3, 4), lax.rem(t + 2, 4)

    def pass_round(source, blocks, first, second, first_sent, second_sent):
        remote(source, blocks.at[t], first_sent, first.at[0], me, up).start()
        remote(source, blocks.at[t], first_sent, first.at[1], me, down).start()

        def pass_on():
            wait_bytes(blocks.at[down], first.at[0])
            half = blocks.at[down, pl.ds(0, 128)]
            remote(half, half, second_sent, second, me, up).start()
            wait_bytes(blocks.at[up], first.at[1])
            half = blocks.at[up, pl.ds(128, 128)]
            remote(half, half, second_sent, second, me, down).start()

        return pass_on

    own_rows = pltpu.make_async_copy(row_own, rows.at[t], own_sem)
    own_rows.start()
    pass_rows_on = pass_round(row_own, rows, rows_sem, rows_last, rows_sent, rows_sent2)

    pltpu.make_async_copy(cols_in, cols, cols_sem).start()
    small = [(row_esc_in, row_esc), (col_esc_in, col_esc), (row_eig_in, row_eig), (col_eig_in, col_eig)]
    small = [pltpu.make_async_copy(a, b, small_sem.at[i]) for i, (a, b) in enumerate(small)]
    for copy in small:
        copy.start()

    def offsets(k):
        a = lax.rem(k + 1, 4)
        return a, lax.rem(k // 4 + a, 4)

    def block_rows(ref, index, part):
        return ref.at[index, pl.ds(pl.multiple_of(part * 256, 256), 256)]

    def scatter_plane(k, carry):
        kk, dest_core = lax.rem(k, 16), 1 - k // 16
        a, b = offsets(kk)
        dx, dy = lax.rem(x + a, 4), lax.rem(y + b, 4)
        mine = (dx == x) & (dy == y) & (dest_core == core)
        relay = layer_at(dx, dy, zlo, dest_core)
        slot = core * 16 + kk
        for dz in range(2):
            layer = layer_at(dx, dy, dz, dest_core)
            final = 2 * x + dz == z
            target = block_rows(block, my_block, t)

            @pl.when(jnp.logical_not(mine) & jnp.logical_not(final))
            def _():
                remote(
                    grad.at[layer], mid.at[slot, dz], sent, relay_sem.at[slot, dz], relay, t
                ).start()

            @pl.when(jnp.logical_not(mine) & final)
            def _():
                remote(grad.at[layer], target, sent, block_sem.at[my_block], relay, t).start()

            @pl.when(mine & jnp.logical_not(final))
            def _():
                remote(grad.at[layer], target, sent, block_sem.at[my_block], layer, x).start()

            @pl.when(mine & final)
            def _():
                pltpu.make_async_copy(grad.at[layer], target, block_sem.at[my_block]).start()

        return carry

    lax.fori_loop(0, 32, scatter_plane, 0)

    def forward(k, carry):
        kk, source_core = k // 2, lax.rem(core + k, 2)
        a, b = offsets(kk)
        sx, sy = lax.rem(x - a + 4, 4), lax.rem(y - b + 4, 4)
        mine = (sx == x) & (sy == y) & (source_core == core)
        slot = source_core * 16 + kk
        index = zlo * 8 + sy * 2 + source_core
        for dz in range(2):

            @pl.when(jnp.logical_not(mine) & (2 * sx + dz != z))
            def _():
                held = mid.at[slot, dz]
                wait_bytes(held, relay_sem.at[slot, dz])
                remote(
                    held,
                    block_rows(block, index, t),
                    sent,
                    block_sem.at[index],
                    layer_at(x, y, dz, core),
                    sx,
                ).start()

        return carry

    lax.fori_loop(0, core * 8, forward, 0)
    pass_rows_on()
    @pl.when(core == 0)
    def _():
        pl.semaphore_wait(go_sem, 1)

    lax.fori_loop(core * 8, 32, forward, 0)

    for copy in small:
        copy.wait()
    row_e = jnp.broadcast_to(row_esc[...], (1, 256))
    col_e = jnp.broadcast_to(col_esc[...], (1, 256))
    row_base, col_base = inverse_fourth_root(row_e), inverse_fourth_root(col_e)
    row_coef = inverse_fourth_root(row_eig[...] + row_e) - row_base
    col_coef = inverse_fourth_root(col_eig[...] + col_e) - col_base
    coef_t[...] = jnp.transpose(jnp.broadcast_to(row_coef, (256, 256)))

    own_rows.wait()
    wait_bytes(rows.at[across], rows_last)
    wait_bytes(cols, cols_sem)
    for r in range(4):
        rows_t[:, 256 * r : 256 * (r + 1)] = jnp.transpose(rows[r].astype(F32)).astype(BF16)

    middle[...] = jnp.zeros_like(middle)
    grad_acc[...] = jnp.zeros_like(grad_acc)
    shift = lax.rem(x - t + 4, 4)

    def project(i, carry):
        sy = lax.rem(y - shift - i // 2 + 8, 4)
        p = lax.rem(i, 2) * 4 + sy
        for half in range(2):
            wait_bytes(block.at[2 * p + half], block_sem.at[2 * p + half])
        pair = jnp.concatenate([block[2 * p], block[2 * p + 1]], axis=1)
        proj = jnp.dot(rows_t[...], pair, preferred_element_type=F32)
        scaled[p] = (coef_t[...] * proj).astype(BF16)
        column = cols[pl.ds(pl.multiple_of(p * 256, 256), 256), :]
        for r in range(4):
            piece = pair[256 * r : 256 * (r + 1)]
            middle[r] += jnp.dot(piece, column, preferred_element_type=F32)
            grad_acc[...] += fold(piece.astype(F32))

        @pl.when((core == 1) & (i == GO_AFTER))
        def _():
            pl.semaphore_signal(go_sem, inc=1, device_id=(me - 1, t), device_id_type=MESH)

        return carry

    lax.fori_loop(0, 8, project, 0)

    far = middle[across].astype(BF16)
    mid_far[...] = far
    remote(mid_far.at[pl.ds(0, 128)], mid_via.at[0], far_sent, far_sem.at[0], me, down).start()
    remote(mid_far.at[pl.ds(128, 128)], mid_via.at[1], far_sent, far_sem.at[1], me, up).start()
    wait_bytes(mid_via.at[0], far_sem.at[0])
    wait_bytes(mid_via.at[1], far_sem.at[1])
    mid_send[0, 0:128] = (middle[down, 0:128] + mid_via[0].astype(F32)).astype(BF16)
    mid_send[0, 128:256] = middle[down, 128:256].astype(BF16)
    mid_send[1, 0:128] = middle[up, 0:128].astype(BF16)
    mid_send[1, 128:256] = (middle[up, 128:256] + mid_via[1].astype(F32)).astype(BF16)
    remote(mid_send.at[0], mid_recv.at[0], part_sent, part_sem, me, down).start()
    remote(mid_send.at[1], mid_recv.at[1], part_sent, part_sem, me, up).start()
    wait_bytes(mid_recv, part_sem)
    mid_all[t] = (middle[t] + mid_recv[0].astype(F32) + mid_recv[1].astype(F32)).astype(BF16)
    pass_middle_on = pass_round(mid_all.at[t], mid_all, full_sem, full_last, full_sent, full_sent2)
    pass_middle_on()
    wait_bytes(mid_all.at[across], full_last)

    core_mat = jnp.zeros((256, 256), F32)
    for r in range(4):
        core_mat += jnp.dot(
            rows_t[:, 256 * r : 256 * (r + 1)], mid_all[r], preferred_element_type=F32
        )
    core_mat = (coef_t[...] * core_mat).astype(BF16)
    for r in range(4):
        mixed = row_base * mid_all[r].astype(F32) + jnp.dot(
            rows[r], core_mat, preferred_element_type=F32
        )
        left[r] = (mixed * col_coef).astype(BF16)

    both_base = row_base * col_base
    norm_send[0] = grad_acc[...]
    norm_send[1] = jnp.zeros((8, 128), F32)

    def order(k):
        return lax.rem(zlo + k, 2) * 4 + lax.rem(y + k // 2, 4)

    def send_pair(i, carry):
        p = order(i)
        for h in range(2):
            index = 2 * p + lax.rem(core + h, 2)
            layer = t * 16 + index
            for o in range(4):
                part = lax.rem(t + o + 1, 4)
                piece = block_rows(ready, index, part)
                own = (layer == me) & (part == t)

                @pl.when(jnp.logical_not(own))
                def _():
                    remote(piece, out.at[me], out_sent, out_sem.at[my_group], layer, part).start()

                @pl.when(own)
                def _():
                    pltpu.make_async_copy(piece, out.at[me], out_sem.at[my_group]).start()

        return carry

    def update(i, carry):
        p = order(i)
        column = cols[pl.ds(pl.multiple_of(p * 256, 256), 256), :]
        for r in range(4):
            span = slice(256 * r, 256 * (r + 1))
            value = jnp.dot(rows[r], scaled[p], preferred_element_type=F32) * col_base
            value += lax.dot_general(
                left[r], column, (((1,), (1,)), ((), ())), preferred_element_type=F32
            )
            held = jnp.concatenate([block[2 * p, span], block[2 * p + 1, span]], axis=1)
            value += both_base * held.astype(F32)
            ready[2 * p, span] = value[:, :128].astype(BF16)
            ready[2 * p + 1, span] = value[:, 128:].astype(BF16)
            norm_send[1] += fold(value)

        @pl.when((i > 0) & (i <= EARLY))
        def _():
            send_pair(i - 1, 0)

        return carry

    lax.fori_loop(0, 8, update, 0)
    for o in range(1, 4):
        remote(
            norm_send, norm_recv.at[3 - o], norm_sent, norm_sem, me, lax.rem(t + o, 4)
        ).start()
    lax.fori_loop(EARLY, LATE, send_pair, 0)
    wait_bytes(norm_recv, norm_sem)
    sums = norm_send[...] + norm_recv[0] + norm_recv[1] + norm_recv[2]
    grad_sq = jnp.sum(sums[0], keepdims=True)
    update_sq = jnp.sum(sums[1], keepdims=True)
    factor = jnp.sqrt((grad_sq + 1.0) / (update_sq + 1.0))
    factor_out[...] = jnp.broadcast_to(factor, (8, 128))
    wait_bytes(norm_recv, norm_sent)

    def give(i, carry):
        layer, part = t * 16 + lax.rem(my_block + i // 4, 16), lax.rem(t + i + 1, 4)
        own = (layer == me) & (part == t)

        @pl.when(jnp.logical_not(own))
        def _():
            remote(
                factor_out.at[pl.ds(0, 1)],
                factor_in.at[me, pl.ds(0, 1)],
                factor_sent,
                factor_sem.at[core],
                layer,
                part,
            ).start()

        @pl.when(own)
        def _():
            pltpu.make_async_copy(
                factor_out.at[pl.ds(0, 1)], factor_in.at[me, pl.ds(0, 1)], factor_sem.at[core]
            ).start()

        return carry

    lax.fori_loop(0, 64, give, 0)
    lax.fori_loop(LATE, 8, send_pair, 0)

    def scale(i, carry):
        @pl.when(lax.rem(i, 8) == 0)
        def _():
            wait_bytes(factor_in.at[pl.ds(0, 32), pl.ds(0, 1)], factor_sem.at[1 - i // 8])

        wait_bytes(out.at[pl.ds(0, 4)], out_sem.at[i])
        for j in range(4):
            layer = layer_at(lax.rem(i // 2, 4), j, lax.rem(i, 2), 1 - i // 8)
            out[layer] = (out[layer].astype(F32) * factor_in[layer, 0:1]).astype(BF16)
        return carry

    lax.fori_loop(0, 16, scale, 0)
    wait_bytes(mid, sent)
    wait_bytes(mid.at[pl.ds(0, 27)], sent)
    wait_bytes(rows.at[pl.ds(0, 2)], rows_sent)
    wait_bytes(rows.at[0], rows_sent2)
    wait_bytes(mid_far, far_sent)
    wait_bytes(mid_recv, part_sent)
    wait_bytes(mid_recv, full_sent)
    wait_bytes(mid_far, full_sent2)

    @pl.when(home)
    def _():
        wait_bytes(out.at[pl.ds(0, 63)], out_sent)
        wait_bytes(factor_in.at[pl.ds(0, 63), pl.ds(0, 1)], factor_sent)

    @pl.when(jnp.logical_not(home))
    def _():
        wait_bytes(out, out_sent)
        wait_bytes(factor_in.at[:, pl.ds(0, 1)], factor_sent)


def body(gradient, row_basis, column_basis, row_eigen, column_eigen, row_escape, column_escape):
    dma = pltpu.SemaphoreType.DMA
    vmem = pl.BlockSpec(memory_space=pltpu.VMEM)
    hbm = pl.BlockSpec(memory_space=pltpu.HBM)
    return pl.pallas_call(
        kernel,
        out_shape=pltpu.VMEM((64, 256, 128), BF16),
        in_specs=[hbm] * 7,
        out_specs=vmem,
        scratch_shapes=[
            pltpu.VMEM((16, 1024, 128), BF16),
            pltpu.VMEM((32, 2, 256, 128), BF16),
            pltpu.VMEM((4, 256, 256), BF16),
            pltpu.VMEM((256, 1024), BF16),
            pltpu.VMEM((256, 256), F32),
            pltpu.VMEM((8, 256, 256), BF16),
            pltpu.VMEM((4, 256, 256), F32),
            pltpu.VMEM((256, 256), BF16),
            pltpu.VMEM((2, 128, 256), BF16),
            pltpu.VMEM((2, 256, 256), BF16),
            pltpu.VMEM((2, 256, 256), BF16),
            pltpu.VMEM((4, 256, 256), BF16),
            pltpu.VMEM((4, 256, 256), BF16),
            pltpu.VMEM((16, 1024, 128), BF16),
            pltpu.VMEM((8, 128), F32),
            pltpu.VMEM((64, 8, 128), F32),
            pltpu.VMEM((2, 8, 128), F32),
            pltpu.VMEM((3, 2, 8, 128), F32),
            pltpu.VMEM((8, 128), F32),
            pltpu.VMEM((2048, 256), BF16),
            pltpu.VMEM((1, 1), F32),
            pltpu.VMEM((1, 1), F32),
            pltpu.VMEM((1, 256), F32),
            pltpu.VMEM((1, 256), F32),
            dma,
            dma((32, 2)),
            dma((16,)),
            dma((2,)),
            dma,
            dma,
            dma,
            dma((2,)),
            dma,
            dma,
            dma,
            dma((16,)),
            dma,
            dma((2,)),
            dma,
            pltpu.SemaphoreType.REGULAR,
            dma,
            dma,
            dma,
            dma,
            dma((2,)),
            dma,
            dma,
            dma,
            dma((4,)),
        ],
        compiler_params=pltpu.CompilerParams(
            collective_id=0, has_side_effects=True, vmem_limit_bytes=56 * 1024 * 1024
        ),
        name="sketchy",
    )(
        row_escape.reshape(1, 1),
        column_escape.reshape(1, 1),
        gradient,
        row_basis.reshape(256, 256),
        column_basis.reshape(2048, 256),
        row_eigen,
        column_eigen,
    )


def solution(mesh):
    in_specs = (
        P(None, "tensor", "layer"),
        P("layer", "tensor", None),
        P("layer", "tensor", None),
        P("layer", None),
        P("layer", None),
        P("layer"),
        P("layer"),
    )
    out_specs = P(None, "tensor", "layer")
    return jax.shard_map(body, mesh=mesh, in_specs=in_specs, out_specs=out_specs, check_vma=False)
```

```python
import jax
import jax.numpy as jnp
from jax import lax
from jax.experimental import pallas as pl
from jax.experimental.pallas import tpu as pltpu
from jax.sharding import PartitionSpec as P

MESH = pl.DeviceIdType.MESH
GO_AFTER = 4
EARLY, LATE = 3, 7
F32 = jnp.float32
BF16 = jnp.bfloat16


def layer_at(x, y, zlo, core):
    return ((x * 2 + zlo) * 4 + y) * 2 + core


def remote(src, dst, send, recv, layer, tensor):
    return pltpu.make_async_remote_copy(
        src_ref=src,
        dst_ref=dst,
        send_sem=send,
        recv_sem=recv,
        device_id=(layer, tensor),
        device_id_type=MESH,
    )


def wait_bytes(ref, sem):
    pltpu.make_async_copy(ref, ref, sem).wait()


def inverse_fourth_root(value):
    return lax.rsqrt(jnp.sqrt(value))


def fold(value):
    rows, cols = value.shape
    parts = jnp.sum((value * value).reshape(rows // 8, 8, cols), axis=0)
    return sum(parts[:, c : c + 128] for c in range(0, cols, 128))


def kernel(
    row_esc_in,
    col_esc_in,
    grad,
    row_own,
    cols_in,
    row_eig_in,
    col_eig_in,
    out,
    block,
    mid,
    rows,
    rows_t,
    coef_t,
    scaled,
    middle,
    mid_far,
    mid_via,
    mid_send,
    mid_recv,
    mid_all,
    left,
    ready,
    factor_out,
    factor_in,
    norm_send,
    norm_recv,
    grad_acc,
    cols,
    row_esc,
    col_esc,
    row_eig,
    col_eig,
    sent,
    relay_sem,
    block_sem,
    rows_sem,
    rows_sent,
    part_sem,
    part_sent,
    full_sem,
    full_sent,
    norm_sem,
    norm_sent,
    out_sem,
    out_sent,
    factor_sem,
    factor_sent,
    go_sem,
    cols_sem,
    own_sem,
    rows_last,
    rows_sent2,
    far_sem,
    far_sent,
    full_last,
    full_sent2,
    small_sem,
):
    me, t = lax.axis_index("layer"), lax.axis_index("tensor")
    x, zlo, y, core = me // 16, lax.rem(me // 8, 2), lax.rem(me // 2, 4), lax.rem(me, 2)
    z = 2 * t + zlo
    my_block = lax.rem(me, 16)
    home = t == x
    my_group = ((1 - core) * 4 + x) * 2 + zlo

    barrier = pltpu.get_barrier_semaphore()

    def greet_plane(i, carry):
        d = lax.rem((x * 4 + y) * 2 + core + i, 32)
        pl.semaphore_signal(
            barrier,
            inc=1,
            device_id=(layer_at(d // 8, lax.rem(d // 2, 4), zlo, lax.rem(d, 2)), t),
            device_id_type=MESH,
        )
        return carry

    def greet_ring(i, carry):
        dz = lax.rem(z + i, 8)
        pl.semaphore_signal(
            barrier,
            inc=1,
            device_id=(layer_at(x, y, lax.rem(dz, 2), core), dz // 2),
            device_id_type=MESH,
        )
        return carry

    lax.fori_loop(1, 8, greet_ring, 0, unroll=True)
    lax.fori_loop(1, 32, greet_plane, 0, unroll=True)
    pl.semaphore_wait(barrier, 38)

    up, down, across = lax.rem(t + 1, 4), lax.rem(t + 3, 4), lax.rem(t + 2, 4)

    def pass_round(source, blocks, first, second, first_sent, second_sent):
        remote(source, blocks.at[t], first_sent, first.at[0], me, up).start()
        remote(source, blocks.at[t], first_sent, first.at[1], me, down).start()

        def pass_on():
            wait_bytes(blocks.at[down], first.at[0])
            half = blocks.at[down, pl.ds(0, 128)]
            remote(half, half, second_sent, second, me, up).start()
            wait_bytes(blocks.at[up], first.at[1])
            half = blocks.at[up, pl.ds(128, 128)]
            remote(half, half, second_sent, second, me, down).start()

        return pass_on

    own_rows = pltpu.make_async_copy(row_own, rows.at[t], own_sem)
    own_rows.start()
    pass_rows_on = pass_round(row_own, rows, rows_sem, rows_last, rows_sent, rows_sent2)

    pltpu.make_async_copy(cols_in, cols, cols_sem).start()
    small = [(row_esc_in, row_esc), (col_esc_in, col_esc), (row_eig_in, row_eig), (col_eig_in, col_eig)]
    small = [pltpu.make_async_copy(a, b, small_sem.at[i]) for i, (a, b) in enumerate(small)]
    for copy in small:
        copy.start()

    def offsets(k):
        a = lax.rem(k + 1, 4)
        return a, lax.rem(k // 4 + a, 4)

    def block_rows(ref, index, part):
        return ref.at[index, pl.ds(pl.multiple_of(part * 256, 256), 256)]

    def scatter_plane(k, carry):
        kk, dest_core = lax.rem(k, 16), 1 - k // 16
        a, b = offsets(kk)
        dx, dy = lax.rem(x + a, 4), lax.rem(y + b, 4)
        mine = (dx == x) & (dy == y) & (dest_core == core)
        relay = layer_at(dx, dy, zlo, dest_core)
        slot = core * 16 + kk
        for dz in range(2):
            layer = layer_at(dx, dy, dz, dest_core)
            final = 2 * x + dz == z
            target = block_rows(block, my_block, t)

            @pl.when(jnp.logical_not(mine) & jnp.logical_not(final))
            def _():
                remote(
                    grad.at[layer], mid.at[slot, dz], sent, relay_sem.at[slot, dz], relay, t
                ).start()

            @pl.when(jnp.logical_not(mine) & final)
            def _():
                remote(grad.at[layer], target, sent, block_sem.at[my_block], relay, t).start()

            @pl.when(mine & jnp.logical_not(final))
            def _():
                remote(grad.at[layer], target, sent, block_sem.at[my_block], layer, x).start()

            @pl.when(mine & final)
            def _():
                pltpu.make_async_copy(grad.at[layer], target, block_sem.at[my_block]).start()

        return carry

    lax.fori_loop(0, 32, scatter_plane, 0)

    def forward(k, carry):
        kk, source_core = k // 2, lax.rem(core + k, 2)
        a, b = offsets(kk)
        sx, sy = lax.rem(x - a + 4, 4), lax.rem(y - b + 4, 4)
        mine = (sx == x) & (sy == y) & (source_core == core)
        slot = source_core * 16 + kk
        index = zlo * 8 + sy * 2 + source_core
        for dz in range(2):

            @pl.when(jnp.logical_not(mine) & (2 * sx + dz != z))
            def _():
                held = mid.at[slot, dz]
                wait_bytes(held, relay_sem.at[slot, dz])
                remote(
                    held,
                    block_rows(block, index, t),
                    sent,
                    block_sem.at[index],
                    layer_at(x, y, dz, core),
                    sx,
                ).start()

        return carry

    lax.fori_loop(0, core * 8, forward, 0)
    pass_rows_on()
    @pl.when(core == 0)
    def _():
        pl.semaphore_wait(go_sem, 1)

    lax.fori_loop(core * 8, 32, forward, 0)

    for copy in small:
        copy.wait()
    row_e = jnp.broadcast_to(row_esc[...], (1, 256))
    col_e = jnp.broadcast_to(col_esc[...], (1, 256))
    row_base, col_base = inverse_fourth_root(row_e), inverse_fourth_root(col_e)
    row_coef = inverse_fourth_root(row_eig[...] + row_e) - row_base
    col_coef = inverse_fourth_root(col_eig[...] + col_e) - col_base
    coef_t[...] = jnp.transpose(jnp.broadcast_to(row_coef, (256, 256)))

    own_rows.wait()
    wait_bytes(rows.at[across], rows_last)
    wait_bytes(cols, cols_sem)
    for r in range(4):
        rows_t[:, 256 * r : 256 * (r + 1)] = jnp.transpose(rows[r].astype(F32)).astype(BF16)

    middle[...] = jnp.zeros_like(middle)
    grad_acc[...] = jnp.zeros_like(grad_acc)
    shift = lax.rem(x - t + 4, 4)

    def project(i, carry):
        sy = lax.rem(y - shift - i // 2 + 8, 4)
        p = lax.rem(i, 2) * 4 + sy
        for half in range(2):
            wait_bytes(block.at[2 * p + half], block_sem.at[2 * p + half])
        pair = jnp.concatenate([block[2 * p], block[2 * p + 1]], axis=1)
        proj = jnp.dot(rows_t[...], pair, preferred_element_type=F32)
        scaled[p] = (coef_t[...] * proj).astype(BF16)
        column = cols[pl.ds(pl.multiple_of(p * 256, 256), 256), :]
        for r in range(4):
            piece = pair[256 * r : 256 * (r + 1)]
            middle[r] += jnp.dot(piece, column, preferred_element_type=F32)
            grad_acc[...] += fold(piece.astype(F32))

        @pl.when((core == 1) & (i == GO_AFTER))
        def _():
            pl.semaphore_signal(go_sem, inc=1, device_id=(me - 1, t), device_id_type=MESH)

        return carry

    lax.fori_loop(0, 8, project, 0)

    spans = (slice(0, 128), slice(128, 256))
    for h in range(2):
        mid_far[h] = middle[across, :, spans[h]].astype(BF16)
        mid_send[h, 0, 128:256] = middle[down, 128:256, spans[h]].astype(BF16)
        mid_send[h, 1, 0:128] = middle[up, 0:128, spans[h]].astype(BF16)
        for d, peer in ((0, down), (1, up)):
            half = mid_far.at[h, pl.ds(128 * d, 128)]
            remote(half, mid_via.at[h, d], far_sent, far_sem.at[h, d], me, peer).start()
    for h in range(2):
        wait_bytes(mid_via.at[h, 0], far_sem.at[h, 0])
        wait_bytes(mid_via.at[h, 1], far_sem.at[h, 1])
        mid_send[h, 0, 0:128] = (middle[down, 0:128, spans[h]] + mid_via[h, 0].astype(F32)).astype(BF16)
        mid_send[h, 1, 128:256] = (middle[up, 128:256, spans[h]] + mid_via[h, 1].astype(F32)).astype(BF16)
        for d, peer in ((0, down), (1, up)):
            remote(mid_send.at[h, d], mid_recv.at[h, d], part_sent, part_sem.at[h], me, peer).start()
    finish = []
    for h in range(2):
        wait_bytes(mid_recv.at[h], part_sem.at[h])
        total = middle[t, :, spans[h]] + mid_recv[h, 0].astype(F32) + mid_recv[h, 1].astype(F32)
        mid_all[h, t] = total.astype(BF16)
        finish.append(
            pass_round(
                mid_all.at[h, t], mid_all.at[h], full_sem.at[h], full_last.at[h], full_sent, full_sent2
            )
        )
    for pass_middle_on in finish:
        pass_middle_on()
    for h in range(2):
        wait_bytes(mid_all.at[h, across], full_last.at[h])
    whole = [jnp.concatenate([mid_all[0, r], mid_all[1, r]], axis=1) for r in range(4)]

    core_mat = jnp.zeros((256, 256), F32)
    for r in range(4):
        core_mat += jnp.dot(
            rows_t[:, 256 * r : 256 * (r + 1)], whole[r], preferred_element_type=F32
        )
    core_mat = (coef_t[...] * core_mat).astype(BF16)
    for r in range(4):
        mixed = row_base * whole[r].astype(F32) + jnp.dot(
            rows[r], core_mat, preferred_element_type=F32
        )
        left[r] = (mixed * col_coef).astype(BF16)

    both_base = row_base * col_base
    norm_send[0] = grad_acc[...]
    norm_send[1] = jnp.zeros((8, 128), F32)

    def order(k):
        return lax.rem(zlo + k, 2) * 4 + lax.rem(y + k // 2, 4)

    def send_pair(i, carry):
        p = order(i)
        for h in range(2):
            index = 2 * p + lax.rem(core + h, 2)
            layer = t * 16 + index
            for o in range(4):
                part = lax.rem(t + o + 1, 4)
                piece = block_rows(ready, index, part)
                own = (layer == me) & (part == t)

                @pl.when(jnp.logical_not(own))
                def _():
                    remote(piece, out.at[me], out_sent, out_sem.at[my_group], layer, part).start()

                @pl.when(own)
                def _():
                    pltpu.make_async_copy(piece, out.at[me], out_sem.at[my_group]).start()

        return carry

    def update(i, carry):
        p = order(i)
        column = cols[pl.ds(pl.multiple_of(p * 256, 256), 256), :]
        for r in range(4):
            span = slice(256 * r, 256 * (r + 1))
            value = jnp.dot(rows[r], scaled[p], preferred_element_type=F32) * col_base
            value += lax.dot_general(
                left[r], column, (((1,), (1,)), ((), ())), preferred_element_type=F32
            )
            held = jnp.concatenate([block[2 * p, span], block[2 * p + 1, span]], axis=1)
            value += both_base * held.astype(F32)
            ready[2 * p, span] = value[:, :128].astype(BF16)
            ready[2 * p + 1, span] = value[:, 128:].astype(BF16)
            norm_send[1] += fold(value)

        @pl.when((i > 0) & (i <= EARLY))
        def _():
            send_pair(i - 1, 0)

        return carry

    lax.fori_loop(0, 8, update, 0)
    for o in range(1, 4):
        remote(
            norm_send, norm_recv.at[3 - o], norm_sent, norm_sem, me, lax.rem(t + o, 4)
        ).start()
    lax.fori_loop(EARLY, LATE, send_pair, 0)
    wait_bytes(norm_recv, norm_sem)
    sums = norm_send[...] + norm_recv[0] + norm_recv[1] + norm_recv[2]
    grad_sq = jnp.sum(sums[0], keepdims=True)
    update_sq = jnp.sum(sums[1], keepdims=True)
    factor = jnp.sqrt((grad_sq + 1.0) / (update_sq + 1.0))
    factor_out[...] = jnp.broadcast_to(factor, (8, 128))
    wait_bytes(norm_recv, norm_sent)

    def give(i, carry):
        layer, part = t * 16 + lax.rem(my_block + i // 4, 16), lax.rem(t + i + 1, 4)
        own = (layer == me) & (part == t)

        @pl.when(jnp.logical_not(own))
        def _():
            remote(
                factor_out.at[pl.ds(0, 1)],
                factor_in.at[me, pl.ds(0, 1)],
                factor_sent,
                factor_sem.at[core],
                layer,
                part,
            ).start()

        @pl.when(own)
        def _():
            pltpu.make_async_copy(
                factor_out.at[pl.ds(0, 1)], factor_in.at[me, pl.ds(0, 1)], factor_sem.at[core]
            ).start()

        return carry

    lax.fori_loop(0, 64, give, 0)
    lax.fori_loop(LATE, 8, send_pair, 0)

    def scale(i, carry):
        @pl.when(lax.rem(i, 8) == 0)
        def _():
            wait_bytes(factor_in.at[pl.ds(0, 32), pl.ds(0, 1)], factor_sem.at[1 - i // 8])

        wait_bytes(out.at[pl.ds(0, 4)], out_sem.at[i])
        for j in range(4):
            layer = layer_at(lax.rem(i // 2, 4), j, lax.rem(i, 2), 1 - i // 8)
            out[layer] = (out[layer].astype(F32) * factor_in[layer, 0:1]).astype(BF16)
        return carry

    lax.fori_loop(0, 16, scale, 0)
    wait_bytes(mid, sent)
    wait_bytes(mid.at[pl.ds(0, 27)], sent)
    wait_bytes(rows.at[pl.ds(0, 2)], rows_sent)
    wait_bytes(rows.at[0], rows_sent2)
    wait_bytes(mid_far, far_sent)
    wait_bytes(mid_recv, part_sent)
    wait_bytes(mid_recv, full_sent)
    wait_bytes(mid_far, full_sent2)

    @pl.when(home)
    def _():
        wait_bytes(out.at[pl.ds(0, 63)], out_sent)
        wait_bytes(factor_in.at[pl.ds(0, 63), pl.ds(0, 1)], factor_sent)

    @pl.when(jnp.logical_not(home))
    def _():
        wait_bytes(out, out_sent)
        wait_bytes(factor_in.at[:, pl.ds(0, 1)], factor_sent)


def body(gradient, row_basis, column_basis, row_eigen, column_eigen, row_escape, column_escape):
    dma = pltpu.SemaphoreType.DMA
    vmem = pl.BlockSpec(memory_space=pltpu.VMEM)
    hbm = pl.BlockSpec(memory_space=pltpu.HBM)
    return pl.pallas_call(
        kernel,
        out_shape=pltpu.VMEM((64, 256, 128), BF16),
        in_specs=[hbm] * 7,
        out_specs=vmem,
        scratch_shapes=[
            pltpu.VMEM((16, 1024, 128), BF16),
            pltpu.VMEM((32, 2, 256, 128), BF16),
            pltpu.VMEM((4, 256, 256), BF16),
            pltpu.VMEM((256, 1024), BF16),
            pltpu.VMEM((256, 256), F32),
            pltpu.VMEM((8, 256, 256), BF16),
            pltpu.VMEM((4, 256, 256), F32),
            pltpu.VMEM((2, 256, 128), BF16),
            pltpu.VMEM((2, 2, 128, 128), BF16),
            pltpu.VMEM((2, 2, 256, 128), BF16),
            pltpu.VMEM((2, 2, 256, 128), BF16),
            pltpu.VMEM((2, 4, 256, 128), BF16),
            pltpu.VMEM((4, 256, 256), BF16),
            pltpu.VMEM((16, 1024, 128), BF16),
            pltpu.VMEM((8, 128), F32),
            pltpu.VMEM((64, 8, 128), F32),
            pltpu.VMEM((2, 8, 128), F32),
            pltpu.VMEM((3, 2, 8, 128), F32),
            pltpu.VMEM((8, 128), F32),
            pltpu.VMEM((2048, 256), BF16),
            pltpu.VMEM((1, 1), F32),
            pltpu.VMEM((1, 1), F32),
            pltpu.VMEM((1, 256), F32),
            pltpu.VMEM((1, 256), F32),
            dma,
            dma((32, 2)),
            dma((16,)),
            dma((2,)),
            dma,
            dma((2,)),
            dma,
            dma((2, 2)),
            dma,
            dma,
            dma,
            dma((16,)),
            dma,
            dma((2,)),
            dma,
            pltpu.SemaphoreType.REGULAR,
            dma,
            dma,
            dma,
            dma,
            dma((2, 2)),
            dma,
            dma((2,)),
            dma,
            dma((4,)),
        ],
        compiler_params=pltpu.CompilerParams(
            collective_id=0, has_side_effects=True, vmem_limit_bytes=56 * 1024 * 1024
        ),
        name="sketchy",
    )(
        row_escape.reshape(1, 1),
        column_escape.reshape(1, 1),
        gradient,
        row_basis.reshape(256, 256),
        column_basis.reshape(2048, 256),
        row_eigen,
        column_eigen,
    )


def solution(mesh):
    in_specs = (
        P(None, "tensor", "layer"),
        P("layer", "tensor", None),
        P("layer", "tensor", None),
        P("layer", None),
        P("layer", None),
        P("layer"),
        P("layer"),
    )
    out_specs = P(None, "tensor", "layer")
    return jax.shard_map(body, mesh=mesh, in_specs=in_specs, out_specs=out_specs, check_vma=False)
```
